128 devices in a mesh: row: 8 (over z, core), col: 16 (over x, y).
Axes of the slice: x: 4, y: 4, z: 4, core: 2. Of those that a mesh axis runs over, the one named last changes fastest.
Arguments:
- points: float32 [64, 32768], P(None, ('row', 'col')), may hold values from -10 to 10
- start: float32 [32768], P(('row', 'col')), may hold values from -6 to 6
Outputs:
- basis: float32 [9, 32768], P(None, ('row', 'col'))
- tridiag: float32 [2, 8], replicated
The draws below stay inside these ranges and needn't reach their ends.
All inputs are finite; a program needn't handle non-finite values.
Results may differ from the reference program's by a relative error of at most 0.028.
Values may be sent and summed in bfloat16 or wider, within the bound.
No kernel may reach another device: no remote copies, remote signals or barrier semaphores. Data moves between devices by JAX's collectives and lax.ppermute only.
A program may use at most 64 MiB of HBM per device.

```python
import jax
import jax.numpy as jnp
from jax import lax

F = 64
P_DEV = 256
ITERS = 8
NPTS = 32768


def draw_points(key, part):
    groups = max(NPTS // 128, 1)
    key_centre = jax.random.fold_in(key, 11)
    key_noise = jax.random.fold_in(key, 12)
    key_member = jax.random.fold_in(key, 13)
    member = jax.random.randint(key_member, (NPTS,), 0, groups)
    ramp = jnp.arange(NPTS).astype(jnp.float32) / max(NPTS - 1, 1)
    centres = 2.0 * jnp.clip(jax.random.normal(key_centre, (F, groups), jnp.float32), -2.5, 2.5)
    spread = 1.6 - 1.2 * ramp
    noise = jnp.clip(jax.random.normal(key_noise, (F, NPTS), jnp.float32), -3.0, 3.0) * spread[None, :]
    placed = jnp.take(centres, member, axis=1)
    return (placed + noise).astype(jnp.float32)


def levels(key, dims, split, low, largest):
    gain, own = 1.0, jax.random.fold_in(key, 6)
    for dim, blocks in split:
        heights = jnp.exp(jax.random.uniform(jax.random.fold_in(own, dim), (blocks,), jnp.float32, low / len(split), largest / len(split)))
        gain = gain * jnp.repeat(heights, dims[dim] // blocks).reshape([-1 if axis == dim else 1 for axis in range(len(dims))])
    return gain


def gaussian(key, extent, scale, most, pieces=(), held_as=jnp.bfloat16):
    gain = levels(key, extent, pieces, -0.22, 0.18) if pieces else 1.0
    array = jax.random.normal(key, extent, jnp.float32) * scale * gain
    return jnp.minimum(jnp.maximum(array, -most), most).astype(held_as)


def setup_inputs(seed: int = 0) -> dict:
    arg_keys = jax.random.split(jax.random.key(seed), 3)
    points = draw_points(jax.random.fold_in(arg_keys[2], 71), 0)
    start = gaussian(arg_keys[1], (NPTS,), 1.0, 6.0, ((0, 128),), jnp.float32)
    return dict(points=points, start=start)


def kernel_rows(row_pts, col_pts, col_sq, scale):
    cross = lax.dot_general(row_pts, col_pts, (((0,), (0,)), ((), ())), precision=lax.Precision.HIGHEST, preferred_element_type=jnp.float32)
    row_sq = lax.optimization_barrier(jnp.sum(row_pts * row_pts, axis=0))
    dist = row_sq[:, None] + col_sq[None, :] - 2.0 * cross
    return jnp.exp(-dist * scale).astype(jnp.bfloat16)

def reference(points, start):
    feats = points.shape[0]
    total = points.shape[1]
    scale = 0.5 / feats
    block = 8 * P_DEV
    col_sq = lax.optimization_barrier(jnp.sum(points * points, axis=0))
    blocks = jnp.moveaxis(points.reshape(feats, total // block, block), 1, 0)

    def apply(vec):
        vb = vec.astype(jnp.bfloat16)

        def one(pts):
            return jnp.dot(kernel_rows(pts, points, col_sq, scale), vb, preferred_element_type=jnp.float32)
        return lax.map(one, blocks).reshape(total)
    first = start / jnp.sqrt(jnp.sum(start * start) + 1e-06)
    basis = [first]
    alphas = []
    betas = []
    for step in range(ITERS):
        w = apply(basis[-1])
        stacked = jnp.stack(basis)
        h1 = jnp.dot(stacked, w, precision=lax.Precision.HIGHEST)
        w = w - jnp.dot(h1, stacked, precision=lax.Precision.HIGHEST)
        h2 = jnp.dot(stacked, w, precision=lax.Precision.HIGHEST)
        w = w - jnp.dot(h2, stacked, precision=lax.Precision.HIGHEST)
        alphas.append(h1[step])
        beta = jnp.sqrt(jnp.sum(w * w) + 1e-06)
        betas.append(beta)
        basis.append(w / beta)
    return (jnp.stack(basis), jnp.stack([jnp.stack(alphas), jnp.stack(betas)]))
```

```python
import jax
import jax.numpy as jnp
from jax import lax
from jax.experimental import pallas as pl
from jax.experimental.pallas import tpu as pltpu
from jax.sharding import Mesh
from jax.sharding import PartitionSpec as P

ITERS = 8
FEATS = 64
LANES = 128
OWN = 256
CHIPS = 64
DEVICES = 128
CODE = 12.0
ALL = ("z", "core", "x", "y")
CHIP = ("z", "x", "y")
LOG2E = 1.4426950408889634
ROWS = DEVICES * OWN // LANES
VEC_ROWS = 16
BLOCK = LANES + VEC_ROWS
VMEM = pl.BlockSpec(memory_space=pltpu.VMEM)


def parts_of(x):
    hi = x.astype(jnp.bfloat16)
    rest = x - hi.astype(jnp.float32)
    mid = rest.astype(jnp.bfloat16)
    low = (rest - mid.astype(jnp.float32)).astype(jnp.bfloat16)
    return hi, mid, low


def prepare(points_ref, start_ref, sent_ref, wa_ref, wb_ref):
    x = points_ref[...]
    code = jnp.exp2(x * CODE).T
    sent_ref[:LANES, :] = jnp.concatenate([code[:LANES], code[LANES:]], axis=1).astype(jnp.bfloat16)
    s0, s1, s2 = parts_of(start_ref[...])
    pad = jnp.zeros((VEC_ROWS - 6, LANES), jnp.bfloat16)
    sent_ref[LANES:, :] = jnp.concatenate([s0, s1, s2, pad], axis=0)
    scale = LOG2E / FEATS
    w = x * scale
    whi = w.astype(jnp.bfloat16)
    wlo = (w - whi.astype(jnp.float32)).astype(jnp.bfloat16)
    half = jnp.sum(x * x, axis=0, keepdims=True) * (-0.5 * scale)
    h0, h1, h2 = (jnp.broadcast_to(h.astype(jnp.float32), (FEATS, OWN)) for h in parts_of(half))
    row = lax.broadcasted_iota(jnp.int32, (FEATS, OWN), 0)
    zero = jnp.zeros((FEATS, OWN), jnp.float32)
    own = jnp.where(row == 0, h0, jnp.where(row == 1, h1, jnp.where(row == 2, h2, zero))).astype(jnp.bfloat16)
    wa_ref[...] = jnp.concatenate([whi, whi, wlo, own], axis=0)
    wb_ref[...] = jnp.concatenate([whi, whi, own, wlo], axis=0)


def build(points_ref, wa_ref, wb_ref, out_ref):
    scale = LOG2E / FEATS
    low_half = lax.broadcasted_iota(jnp.int32, (LANES, LANES), 1) < FEATS
    ones = jnp.ones((LANES, LANES), jnp.float32)

    def chip(p, carry):
        code = points_ref[p, :LANES, :].astype(jnp.float32)
        x = jnp.log2(code) * (1.0 / CODE)
        hi = x.astype(jnp.bfloat16).astype(jnp.float32)
        lo = x - hi
        swapped = pltpu.roll(lo, FEATS, 1)
        xx = x * x * (0.5 * scale)
        sq_a = jnp.sum(jnp.where(low_half, xx, 0.0), axis=1, keepdims=True)
        sq_b = jnp.sum(jnp.where(low_half, 0.0, xx), axis=1, keepdims=True)
        a = jnp.concatenate([jnp.where(low_half, hi, swapped), jnp.where(low_half, hi, ones)], axis=1)
        b = jnp.concatenate([jnp.where(low_half, swapped, hi), jnp.where(low_half, ones, hi)], axis=1)
        at = pl.ds(pl.multiple_of((p // 4) * LANES, LANES), LANES)
        s = 2 * (p % 4)
        ea = jnp.dot(a.astype(jnp.bfloat16), wa_ref[...], preferred_element_type=jnp.float32)
        out_ref[s, at, :] = jnp.exp2(ea - sq_a).astype(jnp.bfloat16)
        eb = jnp.dot(b.astype(jnp.bfloat16), wb_ref[...], preferred_element_type=jnp.float32)
        out_ref[s + 1, at, :] = jnp.exp2(eb - sq_b).astype(jnp.bfloat16)
        return carry

    lax.fori_loop(0, CHIPS, chip, 0, unroll=2)


def total(x):
    return jnp.sum(jnp.sum(x.reshape(-1, 8, LANES), axis=0), keepdims=True)


def product(q_ref, mine_ref, other_ref, out_ref):
    core = lax.axis_index("core")
    row = lax.broadcasted_iota(jnp.int32, (8, OWN), 0)
    acc = jnp.zeros((8, OWN), jnp.float32)
    for held, which in ((mine_ref, core), (other_ref, 1 - core)):
        cols = []
        for z in range(4):
            for k in range(4):
                at = pl.multiple_of(z * 64 + which * 32 + 8 * k, 8)
                cols.append(q_ref[pl.ds(at, 8), :])
        q = jnp.concatenate(cols, axis=1).astype(jnp.bfloat16)
        for s in range(8):
            got = jnp.dot(q, held[s], preferred_element_type=jnp.float32)
            acc = acc + jnp.where(row == s, got, 0.0)
    w = jnp.sum(acc, axis=0, keepdims=True)
    w = jnp.concatenate([w[:, :LANES], w[:, LANES:]], axis=0)
    out_ref[...] = jnp.broadcast_to(w[None], out_ref.shape)


def first_step(mine_vec_ref, other_vec_ref, mine_ref, other_ref, q_ref, kept_ref, w_ref):
    kept_ref[...] = jnp.zeros((2, LANES), jnp.float32)
    core = lax.axis_index("core")
    for held, which in ((mine_vec_ref, core), (other_vec_ref, 1 - core)):
        for p in range(CHIPS):
            v = held[p].astype(jnp.float32)
            at = (p // 16) * 64 + which * 32 + (p % 16) * 2
            q_ref[pl.ds(at, 2), :] = v[0:2] + v[2:4] + v[4:6]
    start = q_ref[...]
    q_ref[...] = start / jnp.sqrt(total(start * start) + 1e-6)
    product(q_ref, mine_ref, other_ref, w_ref)


def orthogonalized(w, basis):
    h1 = [total(q[...] * w) for q in basis]
    for h, q in zip(h1, basis):
        w = w - h * q[...]
    h2 = [total(q[...] * w) for q in basis]
    for h, q in zip(h2, basis):
        w = w - h * q[...]
    beta = jnp.sqrt(total(w * w) + 1e-6)
    return w / beta, h1[-1], beta


def note(found_ref, kept_ref, step, alpha, beta):
    width = kept_ref.shape[1]
    lane = lax.broadcasted_iota(jnp.int32, (1, width), 1)
    kept_ref[0:1, :] = jnp.where(lane == step, alpha, found_ref[0:1, :width])
    kept_ref[1:2, :] = jnp.where(lane == step, beta, found_ref[1:2, :width])


def later_step(*refs):
    count = len(refs) - 7
    w_ref, found_ref, basis, mine_ref, other_ref = refs[0], refs[1], refs[2 : 2 + count], refs[2 + count], refs[3 + count]
    q_ref, kept_ref, out_ref = refs[4 + count :]
    q, alpha, beta = orthogonalized(w_ref[...], basis)
    q_ref[...] = q
    note(found_ref, kept_ref, count - 1, alpha, beta)
    product(q_ref, mine_ref, other_ref, out_ref)


def last_step(*refs):
    w_ref, found_ref, basis, own_ref, kept_ref = refs[0], refs[1], refs[2:-2], refs[-2], refs[-1]
    q, alpha, beta = orthogonalized(w_ref[...], basis)
    note(found_ref, kept_ref, len(basis) - 1, alpha, beta)
    z, core, x, y = (lax.axis_index(a) for a in ALL)
    device = ((z * 2 + core) * 4 + x) * 4 + y
    mask = lax.broadcasted_iota(jnp.int32, (ROWS, LANES), 0)
    for i, held in enumerate(basis):
        for h in range(2):
            own_ref[i : i + 1, h * LANES : (h + 1) * LANES] = held[pl.ds(2 * device + h, 1), :]
    for h in range(2):
        row = jnp.where(mask == 2 * device + h, q, 0.0)
        own_ref[len(basis) :, h * LANES : (h + 1) * LANES] = jnp.sum(row, axis=0, keepdims=True)


def exchanged(x, axis):
    return lax.all_to_all(x, axis, 0, 0, tiled=True)


def sent_to_all(x, axis):
    return exchanged(jnp.broadcast_to(x[None], (lax.axis_size(axis), *x.shape)), axis)


def kept(shape, dtype):
    return pltpu.VMEM(shape, dtype)


def call(body, outs, *args, limit=24 * 2**20):
    return pl.pallas_call(
        body,
        out_shape=outs,
        in_specs=[VMEM] * len(args),
        out_specs=[VMEM] * len(outs),
        compiler_params=pltpu.CompilerParams(vmem_limit_bytes=limit),
    )(*args)


def per_device(points, start):
    f32, bf16 = jnp.float32, jnp.bfloat16
    sent, wa, wb = call(
        prepare,
        (
            jax.ShapeDtypeStruct((BLOCK, LANES), bf16),
            jax.ShapeDtypeStruct((OWN, OWN), bf16),
            jax.ShapeDtypeStruct((OWN, OWN), bf16),
        ),
        points,
        start.reshape(2, LANES),
    )
    mine = sent_to_all(sent, CHIP)
    other = lax.ppermute(mine, "core", [(0, 1), (1, 0)])
    slab = kept((8, CHIPS * OWN // 8, OWN), bf16)
    (mine_k,) = call(build, (slab,), mine, wa, wb)
    (other_k,) = call(build, (slab,), other, wa, wb)
    vector = jax.ShapeDtypeStruct((ROWS, LANES), f32)
    pair = jax.ShapeDtypeStruct((2, LANES), f32)
    spread = jax.ShapeDtypeStruct((DEVICES, 2, LANES), f32)
    q, heads, w = call(first_step, (vector, pair, spread), mine[:, LANES:], other[:, LANES:], mine_k, other_k)
    basis = [q]
    for _ in range(ITERS - 1):
        full = exchanged(w, ALL).reshape(ROWS, LANES)
        q, heads, w = call(later_step, (vector, pair, spread), full, heads, *basis, mine_k, other_k)
        basis.append(q)
    full = exchanged(w, ALL).reshape(ROWS, LANES)
    own, heads = call(last_step, (jax.ShapeDtypeStruct((ITERS + 1, OWN), f32), jax.ShapeDtypeStruct((2, ITERS), f32)), full, heads, *basis)
    return own, heads


def solution(mesh):
    torus = Mesh(mesh.devices.reshape(4, 2, 4, 4), ALL)
    return jax.shard_map(
        per_device,
        mesh=torus,
        in_specs=(P(None, ALL), P(ALL)),
        out_specs=(P(None, ALL), P()),
        check_vma=False,
    )
```
